256 devices in a mesh: groups: 2 (over z), dp: 64 (over y, x), mp: 2 (over core).
Axes of the slice: x: 8, y: 8, z: 2, core: 2. Of those that a mesh axis runs over, the one named last changes fastest.
The devices are a block of a 8x8x16 slice.
Arguments:
- tokens: bfloat16 [32768, 8192], P(('groups', 'dp'), 'mp'), parts along dimension 0, may hold values from -6 to 6
- queries: bfloat16 [32768, 8192], P(('groups', 'dp'), 'mp'), parts along dimension 0, may hold values from -384 to 384, as said below
- w_key: bfloat16 [8192, 1024], P('dp', 'mp'), may hold values from -0.0625 to 0.0625
- w_value: bfloat16 [8192, 1024], P('dp', 'mp'), may hold values from -0.0625 to 0.0625
- lengths: int32 [16, 16], P('groups'), parts along dimension 0, may hold values from 1 to 1920, 2048 in all within a row
Outputs:
- attended: bfloat16 [32768, 8192], P(('groups', 'dp'), 'mp'), parts along dimension 0
The draws below stay inside these ranges and needn't reach their ends.
There are 2 independent parts, one for each index of `groups`. The reference program is written for one: setup_inputs(seed, part) draws one part's arguments, and reference() takes and returns one part's arrays. A program takes and returns all parts, laid end to end along the dimension named above; an argument that names none is the same for every part. Nothing has to cross between parts.
Inputs may be any that keep to these rules, and one draw needn't show every extreme that they name: Real-valued queries.
All inputs are finite; a program needn't handle non-finite values.
Results may differ from the reference program's by a relative error of at most 0.0055.
The reference program's roundings to bfloat16 on the way count: a program that leaves them out, or rounds other values in their place, can miss the bound.
Values may be sent and summed in bfloat16 or wider, within the bound.
No kernel may reach another device: no remote copies, remote signals or barrier semaphores. Data moves between devices by JAX's collectives and lax.ppermute only.
A program may use at most 128 MiB of HBM per device.

```python
import math
import jax
import jax.numpy as jnp
import numpy as np
from jax import lax

D = 8192
H = 64
KV = 8
DH = 128
ROW = 2048
SEQ_ROW = 16
KVW = 1024
MOST = 1920
TOKENS = 16384
ROWS = 8


def draw_queries(key, part):
    base = jax.random.normal(jax.random.fold_in(key, 11), (TOKENS, H * DH), jnp.float32)
    return jnp.clip(base, -384.0, 384.0).astype(jnp.bfloat16)


def level_of(stream_key, extent, cuts, least, high):
    def one(dim, shards_of):
        heights = jax.random.uniform(jax.random.fold_in(jax.random.fold_in(stream_key, 6), dim), (shards_of,), jnp.float32, least / len(cuts), high / len(cuts))
        return jnp.repeat(jnp.exp(heights), extent[dim] // shards_of).reshape((-1,) + (1,) * (len(extent) - dim - 1))

    loudness = one(*cuts[0])
    for cut in cuts[1:]:
        loudness = loudness * one(*cut)
    return loudness


def length_profile(amount, total, limit, lean):
    weights = [(1 << 20) // math.isqrt(rank ** lean) + 1 for rank in range(2, amount + 1)]
    rest, given = total - limit - (amount - 1), [1] * (amount - 1)
    while rest > 0:
        free = [i for i in range(amount - 1) if given[i] < limit]
        pool, budget = sum([weights[i] for i in free]), rest
        for i in free:
            addition = min(limit - given[i], max(1, budget * weights[i] // pool), rest)
            given[i] = given[i] + addition
            rest = rest - addition
    return np.array([limit] + given)


def uneven(key, count, total, limit, slope):
    if count == 2:
        one = jax.random.randint(key, (), max(1, total - limit), min(limit, total - 1) + 1)
        return jnp.stack([one, total - one])
    sizes = jnp.asarray(length_profile(count, total, limit, slope), jnp.int32)
    twos = (count - 1) // 2
    source_of, taker = sizes[1:1 + 2 * twos:2], sizes[2:2 + 2 * twos:2]
    margin = jnp.minimum(source_of - 1, limit - taker)
    shifted = jax.random.randint(jax.random.fold_in(key, 1), (twos,), 0, 1 << 20) % (margin + 1)
    sizes = sizes.at[1:1 + 2 * twos:2].set(source_of - shifted).at[2:2 + 2 * twos:2].set(taker + shifted)
    return sizes[jax.random.permutation(jax.random.fold_in(key, 2), count)]


def bell_draw(rng, extent, width, most, cuts=(), kind=jnp.bfloat16):
    array = width * jax.random.normal(rng, extent, jnp.float32)
    if cuts:
        array = array * level_of(rng, extent, cuts, -0.22, 0.18)
    return jnp.clip(array, -most, most).astype(kind)


def setup_inputs(seed: int = 0, part: int = 0) -> dict:
    key_list = jax.random.split(jax.random.key(seed), 6)
    own_keys = jax.random.split(jax.random.fold_in(key_list[5], part), 6)
    return {
        "tokens": bell_draw(own_keys[0], (TOKENS, D), 1.0, 6.0, ((0, 64), (1, 2))),
        "queries": draw_queries(jax.random.fold_in(jax.random.fold_in(key_list[5], part), 71), part),
        "w_key": bell_draw(key_list[2], (D, KVW), D ** -0.5, 0.0625, ((0, 64), (1, 2))),
        "w_value": bell_draw(key_list[3], (D, KVW), D ** -0.5, 0.0625, ((0, 64), (1, 2))),
        "lengths": jax.vmap(lambda own: uneven(own, SEQ_ROW, ROW, MOST, 2))(jax.random.split(own_keys[4], ROWS)).reshape((ROWS, SEQ_ROW)).astype(jnp.int32),
    }


def rotate(values, positions):
    half_dim = values.shape[-1] // 2
    frequency = jnp.power(500000.0, -2.0 * jnp.arange(half_dim, dtype=jnp.float32) / values.shape[-1])
    angles = positions.astype(jnp.float32)[:, None] * frequency[None, :]
    cosine = jnp.cos(angles)[:, None, :]
    sine_part = jnp.sin(angles)[:, None, :]
    first_half = values[..., :half_dim]
    second_half = values[..., half_dim:]
    return jnp.concatenate([first_half * cosine - second_half * sine_part, second_half * cosine + first_half * sine_part], axis=-1)

def sequence_tables(lengths):
    finish = jnp.cumsum(lengths, axis=1)
    offsets = jnp.arange(ROW, dtype=jnp.int32)
    before = finish[:, None, :] <= offsets[None, :, None]
    sequence = lax.optimization_barrier(jnp.sum(before.astype(jnp.int32), axis=2))
    started = lax.optimization_barrier(jnp.sum(jnp.where(before, lengths[:, None, :], 0), axis=2))
    return (sequence, offsets[None, :] - started)

def reference(tokens, queries, w_key, w_value, lengths):
    half_row = ROW // 2
    tokens_rows = jnp.roll(tokens, -half_row, axis=0)
    queries_rows = jnp.roll(queries, -half_row, axis=0)
    sequence, positions = sequence_tables(lengths)
    keys_raw = jnp.dot(tokens_rows, w_key, preferred_element_type=jnp.float32).reshape(TOKENS, KV, DH)
    keys_all = rotate(keys_raw, positions.reshape(TOKENS)).astype(jnp.bfloat16)
    values_all = jnp.dot(tokens_rows, w_value, preferred_element_type=jnp.float32).astype(jnp.bfloat16)
    group_size = H // KV
    scale_factor = 1.0 / math.sqrt(DH)
    query_rows = queries_rows.reshape(ROWS, ROW, KV, group_size, DH)
    key_rows = keys_all.reshape(ROWS, ROW, KV, DH)
    value_rows = values_all.reshape(ROWS, ROW, KV, DH)
    causal = jnp.arange(ROW, dtype=jnp.int32)[None, :] <= jnp.arange(ROW, dtype=jnp.int32)[:, None]

    def one_row(row_items):
        query_row, key_row, value_row, sequence_row = row_items
        scores = jnp.einsum('tkgd,ukd->kgtu', query_row.astype(jnp.float32), key_row.astype(jnp.float32)) * scale_factor
        allowed = causal & (sequence_row[:, None] == sequence_row[None, :])
        masked = jnp.where(allowed, scores, -1e+30)
        row_peak = lax.optimization_barrier(jnp.max(masked, axis=-1, keepdims=True))
        weights = jnp.where(allowed, jnp.exp(masked - row_peak), 0.0)
        probability = (weights / lax.optimization_barrier(jnp.sum(weights, axis=-1, keepdims=True))).astype(jnp.bfloat16)
        mixed_heads = jnp.einsum('kgtu,ukd->tkgd', probability.astype(jnp.float32), value_row.astype(jnp.float32))
        return mixed_heads.reshape(ROW, H * DH).astype(jnp.bfloat16)
    attended = lax.map(one_row, (query_rows, key_rows, value_rows, sequence))
    return jnp.roll(attended.reshape(TOKENS, H * DH), half_row, axis=0)
```

```python
import functools
import math

import jax
import jax.numpy as jnp
from jax import lax
from jax.experimental import pallas as pl
from jax.experimental.pallas import tpu as pltpu
from jax.sharding import PartitionSpec as P

DH = 128
ROW = 2048
HEADS_PER_STEP = 4
STACK = 2
NEG = -1e30


def torus_shift(block, side, dy, dx):
    route = []
    for y in range(side):
        for x in range(side):
            route.append((y * side + x, (y + dy) % side * side + (x + dx) % side))
    return lax.ppermute(block, "dp", route)


def next_on_dp(block):
    count = lax.axis_size("dp")
    return lax.ppermute(block, "dp", [(i, (i + 1) % count) for i in range(count)])


def group_swap(block):
    count = lax.axis_size("groups")
    return lax.ppermute(block, "groups", [(i, i ^ 1) for i in range(count)])


def core_swap(block):
    return lax.ppermute(block, "mp", [(0, 1), (1, 0)])


def join_kernel(side, where_ref, *refs):
    pieces, out = refs[:-1], refs[-1]
    own = where_ref[0]
    rows = pieces[0].shape[0]
    for shift, piece in pieces_with_shift(side, pieces):
        source = lax.rem(own - shift + 2 * side, side)
        out[pl.ds(pl.multiple_of(source * rows, rows), rows), :] = piece[...]


def pieces_with_shift(side, pieces):
    shifts = [0] + list(range(1, side // 2 + 1)) + [-k for k in range(1, side // 2)]
    return list(zip(shifts, pieces))


def join(side, own, pieces):
    rows, columns = pieces[0].shape
    return pl.pallas_call(
        functools.partial(join_kernel, side),
        in_specs=[pl.BlockSpec(memory_space=pltpu.SMEM)]
        + [pl.BlockSpec(memory_space=pltpu.VMEM)] * len(pieces),
        out_specs=pl.BlockSpec(memory_space=pltpu.VMEM),
        out_shape=jax.ShapeDtypeStruct((side * rows, columns), pieces[0].dtype),
        compiler_params=pltpu.CompilerParams(vmem_limit_bytes=8 * 2**20),
        cost_estimate=pl.CostEstimate(
            flops=10**6, bytes_accessed=4 * side * rows * columns, transcendentals=0
        ),
        name="join",
    )(own, *pieces)


def project_kernel(side, key_chunks, value_chunks, sets, final, where_ref, *refs):
    refs = list(refs)
    take = lambda n: [refs.pop(0) for _ in range(n)]
    weights_k = take(len(key_chunks))
    weights_v = take(len(value_chunks))
    tokens = [take(2) for _ in range(sets)]
    sums = [take(2) for _ in range(sets)] if final != "first" else None
    tables = [take(2) for _ in range(sets)] if final == "last" else None
    outs = refs
    y, x, core = where_ref[0], where_ref[1], where_ref[2]
    half = side // 2
    width = weights_k[0].shape[1]
    for s in range(sets):
        own, other = tokens[s]
        key_sum = sums[s][0][...] if sums else None
        value_sum = sums[s][1][...] if sums else None
        add = lambda a, b: b if a is None else a + b
        unit = own.shape[1] // half
        piece = unit // side
        for (shift, lo, hi), w in zip(key_chunks, weights_k):
            row = lax.rem(y - shift + 2 * side, side)
            start = pl.multiple_of(lax.rem(row, half) * unit + lo * piece, piece)
            mine = (lax.div(row, half) == core).astype(jnp.bfloat16)
            a = own[:, pl.ds(start, (hi - lo) * piece)]
            b = other[:, pl.ds(start, (hi - lo) * piece)]
            t = jnp.where(lax.div(row, half) == core, a, b)
            key_sum = add(key_sum, jnp.dot(t, w[...], preferred_element_type=jnp.float32))
        for (shift, lo, hi), w in zip(value_chunks, weights_v):
            column = lax.rem(x - shift + 2 * side, side)
            strips = []
            for row in range(lo, hi):
                start = pl.multiple_of((row % half) * unit + column * piece, piece)
                a = own[:, pl.ds(start, piece)]
                b = other[:, pl.ds(start, piece)]
                strips.append(jnp.where(core == row // half, a, b))
            t = jnp.concatenate(strips, axis=1)
            value_sum = add(value_sum, jnp.dot(t, w[...], preferred_element_type=jnp.float32))
        if final != "last":
            outs[2 * s][...] = key_sum
            outs[2 * s + 1][...] = value_sum
        else:
            cosine, sine = tables[s][0][...], tables[s][1][...]
            rows = key_sum.shape[0]
            for h in range(width // DH):
                k = key_sum[:, h * DH : (h + 1) * DH]
                turned = jnp.concatenate([k[:, DH // 2 :], k[:, : DH // 2]], axis=1)
                outs[s][:rows, h * DH : (h + 1) * DH] = (k * cosine + turned * sine).astype(
                    jnp.bfloat16
                )
            outs[s][rows:, :] = value_sum.astype(jnp.bfloat16)


def project(side, where, key_chunks, value_chunks, tokens, sums=None, tables=None):
    sets = len(tokens)
    rows = tokens[0][0].shape[0]
    width = key_chunks[0][1].shape[1]
    final = "last" if tables is not None else ("first" if sums is None else "middle")
    operands = [w for _, w in key_chunks] + [w for _, w in value_chunks]
    for pair in tokens:
        operands += list(pair)
    if sums is not None:
        for pair in sums:
            operands += list(pair)
    if tables is not None:
        for pair in tables:
            operands += list(pair)
        shapes = [jax.ShapeDtypeStruct((2 * rows, width), jnp.bfloat16)] * sets
    else:
        shapes = [jax.ShapeDtypeStruct((rows, width), jnp.float32)] * (2 * sets)
    depth = sum(w.shape[0] for _, w in key_chunks + value_chunks)
    out = pl.pallas_call(
        functools.partial(
            project_kernel,
            side,
            [c for c, _ in key_chunks],
            [c for c, _ in value_chunks],
            sets,
            final,
        ),
        in_specs=[pl.BlockSpec(memory_space=pltpu.SMEM)]
        + [pl.BlockSpec(memory_space=pltpu.VMEM)] * len(operands),
        out_specs=[pl.BlockSpec(memory_space=pltpu.VMEM)] * len(shapes),
        out_shape=shapes,
        compiler_params=pltpu.CompilerParams(vmem_limit_bytes=40 * 2**20),
        cost_estimate=pl.CostEstimate(
            flops=2 * sets * rows * depth * width,
            bytes_accessed=sum(o.size * o.dtype.itemsize for o in operands),
            transcendentals=0,
        ),
        name="project",
    )(where, *operands)
    if tables is not None:
        return list(out)
    return [(out[2 * s], out[2 * s + 1]) for s in range(sets)]


def attend_kernel(factor, blocks, base_ref, q_ref, bias_ref, *refs):
    keys, values = refs[:blocks], refs[blocks : 2 * blocks]
    o_ref, s_ref = refs[-2], refs[-1]
    rows = q_ref.shape[0]

    def scores(i):
        q = jnp.concatenate(
            [q_ref[:, h * DH : (h + 1) * DH] for h in range(i * STACK, (i + 1) * STACK)], axis=0
        )
        peaks = [None] * STACK
        for b in range(blocks):
            s = lax.dot_general(
                q, keys[b][...], (((1,), (1,)), ((), ())), preferred_element_type=jnp.float32
            )
            for g in range(STACK):
                part = s[g * rows : (g + 1) * rows] + bias_ref[:, b * rows : (b + 1) * rows]
                s_ref[i * STACK + g, :, b * rows : (b + 1) * rows] = part
                for c in range(0, rows, DH):
                    lanes = part[:, c : c + DH]
                    peaks[g] = lanes if peaks[g] is None else jnp.maximum(peaks[g], lanes)
        return [jnp.max(p, axis=1, keepdims=True) for p in peaks]

    def mix(i, peaks):
        total = None
        for b in range(blocks):
            p = jnp.concatenate(
                [
                    jnp.exp2(
                        (s_ref[i * STACK + g, :, b * rows : (b + 1) * rows] - peaks[g]) * factor
                    ).astype(jnp.bfloat16)
                    for g in range(STACK)
                ],
                axis=0,
            )
            v = jnp.concatenate([values[b][...], jnp.ones_like(values[b])], axis=1)
            o = jnp.dot(p, v, preferred_element_type=jnp.float32)
            total = o if total is None else total + o
        out = (total[:, :DH] / total[:, DH:]).astype(jnp.bfloat16)
        for g in range(STACK):
            h = i * STACK + g
            o_ref[:, h * DH : (h + 1) * DH] = out[g * rows : (g + 1) * rows]

    count = HEADS_PER_STEP // STACK
    peaks = scores(0)
    for i in range(count):
        later = scores(i + 1) if i + 1 < count else None
        mix(i, peaks)
        peaks = later


def attend(first_step, queries, bias, pieces, group_size, earlier=None):
    rows, width = queries.shape
    blocks = len(pieces)
    heads = pieces[0].shape[1] // DH * group_size
    steps = heads // HEADS_PER_STEP
    wide = HEADS_PER_STEP * DH
    per = group_size // HEADS_PER_STEP
    key_spec = pl.BlockSpec((rows, DH), lambda h, base: (0, h // per))
    value_spec = pl.BlockSpec((rows, DH), lambda h, base: (1, h // per))
    head_spec = pl.BlockSpec((rows, wide), lambda h, base: (0, base[0] + h))
    in_specs = [head_spec, pl.BlockSpec((rows, blocks * rows), lambda h, base: (0, 0))]
    in_specs += [key_spec] * blocks + [value_spec] * blocks
    operands = [queries, bias, *pieces, *pieces]
    aliases = {}
    kernel = functools.partial(attend_kernel, math.log2(math.e) / math.sqrt(DH), blocks)
    if earlier is not None:
        in_specs.append(pl.BlockSpec(memory_space=pl.ANY))
        operands.append(earlier)
        aliases = {len(operands): 0}
    return pl.pallas_call(
        kernel,
        grid_spec=pltpu.PrefetchScalarGridSpec(
            num_scalar_prefetch=1,
            grid=(steps,),
            in_specs=in_specs,
            out_specs=head_spec,
            scratch_shapes=[pltpu.VMEM((HEADS_PER_STEP, rows, blocks * rows), jnp.float32)],
        ),
        out_shape=jax.ShapeDtypeStruct((rows, width), jnp.bfloat16),
        input_output_aliases=aliases,
        compiler_params=pltpu.CompilerParams(vmem_limit_bytes=40 * 2**20),
        cost_estimate=pl.CostEstimate(
            flops=4 * heads * rows * rows * blocks * DH,
            bytes_accessed=4 * rows * heads * DH + 4 * rows * rows * blocks,
            transcendentals=heads * rows * rows * blocks,
        ),
        name="attend",
    )(first_step, *operands)


def rotation(positions):
    half = DH // 2
    frequency = jnp.power(500000.0, -2.0 * jnp.arange(half, dtype=jnp.float32) / DH)
    angles = positions.astype(jnp.float32)[:, None] * frequency[None, :]
    cosine, sine = jnp.cos(angles), jnp.sin(angles)
    return (
        jnp.concatenate([cosine, cosine], axis=1),
        jnp.concatenate([-sine, sine], axis=1),
    )


def gather_line(side, piece, dy, dx, where):
    pieces = [piece]
    for k in list(range(1, side // 2 + 1)) + [-k for k in range(1, side // 2)]:
        pieces.append(torus_shift(piece, side, dy * k, dx * k))
    return join(side, where, pieces)


def chunk_chain(side, chunk, dy, dx):
    parts = side
    half = side // 2
    rows = chunk.shape[0]
    stages = [[((0, 0, parts), chunk)]]
    forth = back = chunk
    for k in range(1, half):
        forth = torus_shift(forth, side, dy, dx)
        back = torus_shift(back, side, -dy, -dx)
        stages.append([((k, 0, parts), forth), ((-k, 0, parts), back)])
    forth = torus_shift(forth[: rows // 2], side, dy, dx)
    back = torus_shift(back[rows // 2 :], side, -dy, -dx)
    stages.append([((half, 0, parts // 2), forth), ((half, parts // 2, parts), back)])
    return stages


def earlier_blocks(side, block):
    chain = []
    passed = block
    for _ in range(side // 2):
        passed = next_on_dp(passed)
        chain.append(passed)
    above = torus_shift(block, side, 1, 0)
    far = []
    for _ in range(side // 2 - 1):
        above = torus_shift(above, side, 0, -1)
        far.insert(0, above)
    return [block] + chain + far


def per_device(tokens, queries, w_key, w_value, lengths):
    tok_count = tokens.shape[0]
    side = ROW // tok_count
    assert side * side == lax.axis_size("dp") and lax.axis_size("groups") % 2 == 0
    assert lax.axis_size("mp") == 2 and ROW // 2 // tok_count == side // 2
    kv_local = w_key.shape[1] // DH
    group_size = queries.shape[1] // DH // kv_local
    half_width = w_key.shape[1] // 2
    place = lax.axis_index("dp")
    y, x, core = place // side, place % side, lax.axis_index("mp")
    part = lax.axis_index("groups") % 2

    tokens_z = group_swap(tokens)
    tokens_other = core_swap(tokens)

    key_piece = lax.dynamic_slice_in_dim(w_key, part * half_width, half_width, 1)
    value_piece = lax.dynamic_slice_in_dim(w_value, part * half_width, half_width, 1)
    key_chunk = gather_line(side, key_piece, 0, 1, jnp.stack([x]))
    value_chunk = gather_line(side, value_piece, 1, 0, jnp.stack([y]))
    key_stages = chunk_chain(side, key_chunk, 1, 0)
    value_stages = chunk_chain(side, value_chunk, 0, 1)

    all_tokens = tok_count * lax.axis_size("dp")
    first_token = (place * tok_count - ROW // 2 + all_tokens) % all_tokens
    row_index = first_token // ROW
    row_lengths = lax.dynamic_slice_in_dim(lengths, row_index, 1, 0)[0]
    finish = jnp.cumsum(row_lengths)
    own_offsets = first_token - row_index * ROW + jnp.arange(tok_count, dtype=jnp.int32)
    before = finish[None, :] <= own_offsets[:, None]
    started = jnp.sum(jnp.where(before, row_lengths[None, :], 0), axis=1)
    positions = own_offsets - started
    tables = rotation(positions)
    tables_z = rotation(group_swap(positions))
    window = jnp.arange(side * tok_count, dtype=jnp.int32)
    key_offsets = own_offsets[0] - window // tok_count * tok_count + window % tok_count
    allowed = (key_offsets[None, :] >= started[:, None]) & (
        key_offsets[None, :] <= own_offsets[:, None]
    )
    bias = jnp.where(allowed, 0.0, NEG).astype(jnp.float32)

    tokens_z_other = core_swap(tokens_z)
    own_set, z_set = (tokens, tokens_other), (tokens_z, tokens_z_other)
    where = jnp.stack([y, x, core])
    pick = lambda stages, ks: [c for k in ks for c in stages[k]]
    half = side // 2
    early = list(range(half - 1))
    sums = project(
        side, where, pick(key_stages, early), pick(value_stages, early), [own_set]
    ) + project(side, where, pick(key_stages, early), pick(value_stages, early), [z_set])
    late = [half - 1, half]
    kv_own, kv_z = project(
        side,
        where,
        pick(key_stages, late),
        pick(value_stages, late),
        [own_set, z_set],
        sums,
        [tables, tables_z],
    )
    kv_back = group_swap(kv_z)
    steps_half = kv_local // 2 * group_size // HEADS_PER_STEP
    own_pieces = earlier_blocks(side, kv_own)
    back_pieces = earlier_blocks(side, kv_back)
    out = attend(jnp.stack([part * steps_half]), queries, bias, own_pieces, group_size)
    return attend(
        jnp.stack([(1 - part) * steps_half]), queries, bias, back_pieces, group_size, out
    )


def solution(mesh):
    return jax.shard_map(
        per_device,
        mesh=mesh,
        in_specs=(
            P(("groups", "dp"), "mp"),
            P(("groups", "dp"), "mp"),
            P("dp", "mp"),
            P("dp", "mp"),
            P("groups", None),
        ),
        out_specs=P(("groups", "dp"), "mp"),
        check_vma=False,
    )
```

```python
import functools
import math

import jax
import jax.numpy as jnp
from jax import lax
from jax.experimental import pallas as pl
from jax.experimental.pallas import tpu as pltpu
from jax.sharding import PartitionSpec as P

DH = 128
ROW = 2048
HEADS_PER_STEP = 4
STACK = 2
NEG = -1e30


def torus_shift(block, side, dy, dx):
    route = []
    for y in range(side):
        for x in range(side):
            route.append((y * side + x, (y + dy) % side * side + (x + dx) % side))
    return lax.ppermute(block, "dp", route)


def start_backwards(block, side):
    route = []
    for y in range(side):
        for x in range(side):
            down = 1 if x >= side // 2 else 0
            route.append((y * side + x, (y + down) % side * side + (x - 1) % side))
    return lax.ppermute(block, "dp", route)


def next_on_dp(block):
    count = lax.axis_size("dp")
    return lax.ppermute(block, "dp", [(i, (i + 1) % count) for i in range(count)])


def after(values, *others):
    held = lax.optimization_barrier((tuple(values), tuple(others)))
    return list(held[0])


def group_swap(block):
    count = lax.axis_size("groups")
    return lax.ppermute(block, "groups", [(i, i ^ 1) for i in range(count)])


def core_swap(block):
    return lax.ppermute(block, "mp", [(0, 1), (1, 0)])


def join_kernel(side, spans, where_ref, *refs):
    pieces, out, sems = refs[:-2], refs[-2], refs[-1]
    own = where_ref[0]
    rows = out.shape[0] // side
    copies = []
    for piece, shifts in zip(pieces, spans):
        for k, shift in enumerate(shifts):
            source = lax.rem(own - shift + 2 * side, side)
            target = out.at[pl.ds(pl.multiple_of(source * rows, rows), rows), :]
            copies.append(
                pltpu.make_async_copy(
                    piece.at[pl.ds(k * rows, rows), :], target, sems.at[len(copies)]
                )
            )
    for copy in copies:
        copy.start()
    for copy in copies:
        copy.wait()


def join(side, own, pieces, spans):
    columns = pieces[0].shape[1]
    rows = pieces[0].shape[0] // len(spans[0])
    return pl.pallas_call(
        functools.partial(join_kernel, side, spans),
        in_specs=[pl.BlockSpec(memory_space=pltpu.SMEM)]
        + [pl.BlockSpec(memory_space=pl.ANY)] * len(pieces),
        out_specs=pl.BlockSpec(memory_space=pltpu.VMEM),
        out_shape=jax.ShapeDtypeStruct((side * rows, columns), pieces[0].dtype),
        scratch_shapes=[pltpu.SemaphoreType.DMA((side,))],
        compiler_params=pltpu.CompilerParams(vmem_limit_bytes=60 * 2**20),
        cost_estimate=pl.CostEstimate(
            flops=10**6, bytes_accessed=4 * side * rows * columns, transcendentals=0
        ),
        name="join",
    )(own, *pieces)


def project_kernel(side, work, has_sums, final, where_ref, *refs):
    refs = list(refs)
    take = lambda n: [refs.pop(0) for _ in range(n)]
    count = 1 + max(item[0] for keys, values in work for item in keys + values)
    weights = take(count)
    tokens = [take(2) for _ in work]
    sums = [take(2) if has_sums[s] else None for s in range(len(work))]
    tables = [take(2) for _ in work] if final else None
    staged, sems = refs[-2], refs[-1]
    outs = refs[:-2]
    y, x, core = where_ref[0], where_ref[1], where_ref[2]
    half = side // 2
    unit = tokens[0][0].shape[1] // half
    piece = unit // side
    slot, sem = 0, 0
    plan = []
    for s, (keys, values) in enumerate(work):
        own, other = tokens[s]

        def bring(source_half, start, width, slot, lane, sem):
            target = staged.at[slot, :, pl.ds(lane, width)]
            window = pl.ds(pl.multiple_of(start, piece), width)
            for array, test in ((own, source_half == core), (other, source_half != core)):

                @pl.when(test)
                def _():
                    pltpu.make_async_copy(array.at[:, window], target, sems.at[sem]).start()

            return pltpu.make_async_copy(own.at[:, window], target, sems.at[sem])

        for which, items in enumerate((keys, values)):
            for operand, shift, lo, hi in items:
                waits = []
                if which == 0:
                    row = lax.rem(y - shift + 2 * side, side)
                    start = lax.rem(row, half) * unit + lo * piece
                    waits.append(
                        bring(lax.div(row, half), start, (hi - lo) * piece, slot, 0, sem)
                    )
                    sem += 1
                else:
                    column = lax.rem(x - shift + 2 * side, side)
                    for k, row in enumerate(range(lo, hi)):
                        start = (row % half) * unit + column * piece
                        waits.append(
                            bring(row // half, start, piece, slot, k * piece, sem)
                        )
                        sem += 1
                plan.append((s, which, operand, slot, (hi - lo) * piece, waits))
                slot += 1
    totals = [[r[...] for r in sums[s]] if sums[s] else [None, None] for s in range(len(work))]
    for s, which, operand, slot, depth, waits in plan:
        for wait in waits:
            wait.wait()
        product = jnp.dot(
            staged[slot, :, :depth], weights[operand][...], preferred_element_type=jnp.float32
        )
        old = totals[s][which]
        totals[s][which] = product if old is None else old + product
    rows = staged.shape[1]
    for s in range(len(work)):
        key_sum, value_sum = totals[s]
        if not final:
            outs[2 * s][...] = key_sum
            outs[2 * s + 1][...] = value_sum
            continue
        cosine, sine = tables[s][0][...], tables[s][1][...]
        for h in range(key_sum.shape[1] // DH):
            k = key_sum[:, h * DH : (h + 1) * DH]
            turned = jnp.concatenate([k[:, DH // 2 :], k[:, : DH // 2]], axis=1)
            outs[s][:rows, h * DH : (h + 1) * DH] = (k * cosine + turned * sine).astype(
                jnp.bfloat16
            )
        outs[s][rows:, :] = value_sum.astype(jnp.bfloat16)


def project(side, where, work, tokens, sums, tables=None):
    rows = tokens[0][0].shape[0]
    arrays, names = [], []
    for keys, values in work:
        plan = []
        for items in (keys, values):
            plan.append([])
            for (shift, lo, hi), w in items:
                at = next((k for k, a in enumerate(arrays) if a is w), None)
                if at is None:
                    at = len(arrays)
                    arrays.append(w)
                plan[-1].append((at, shift, lo, hi))
        names.append(tuple(plan))
    width = arrays[0].shape[1]
    operands = list(arrays)
    specs = [pl.BlockSpec(memory_space=pltpu.VMEM)] * len(arrays)
    for pair in tokens:
        operands += list(pair)
        specs += [pl.BlockSpec(memory_space=pl.ANY)] * 2
    for pair in list(sums) + list(tables or []):
        if pair is not None:
            operands += list(pair)
            specs += [pl.BlockSpec(memory_space=pltpu.VMEM)] * 2
    if tables is not None:
        shapes = [jax.ShapeDtypeStruct((2 * rows, width), jnp.bfloat16)] * len(work)
    else:
        shapes = [jax.ShapeDtypeStruct((rows, width), jnp.float32)] * (2 * len(work))
    items = [i for keys, values in names for i in keys + values]
    copies = sum(len(keys) + sum(i[3] - i[2] for i in values) for keys, values in names)
    depth = max(a.shape[0] for a in arrays)
    out = pl.pallas_call(
        functools.partial(
            project_kernel, side, names, [p is not None for p in sums], tables is not None
        ),
        in_specs=[pl.BlockSpec(memory_space=pltpu.SMEM)] + specs,
        out_specs=[pl.BlockSpec(memory_space=pltpu.VMEM)] * len(shapes),
        out_shape=shapes,
        scratch_shapes=[
            pltpu.VMEM((len(items), rows, depth), jnp.bfloat16),
            pltpu.SemaphoreType.DMA((copies,)),
        ],
        compiler_params=pltpu.CompilerParams(vmem_limit_bytes=16 * 2**20),
        cost_estimate=pl.CostEstimate(
            flops=2 * rows * depth * width * len(items),
            bytes_accessed=len(items) * depth * (rows + width) * 2,
            transcendentals=0,
        ),
        name="project",
    )(where, *operands)
    if tables is not None:
        return list(out)
    return [(out[2 * s], out[2 * s + 1]) for s in range(len(work))]


def attend_kernel(factor, blocks, base_ref, q_ref, bias_ref, *refs):
    keys, values = refs[:blocks], refs[blocks : 2 * blocks]
    o_ref, s_ref = refs[-2], refs[-1]
    rows = q_ref.shape[0]

    def scores(i):
        q = jnp.concatenate(
            [q_ref[:, h * DH : (h + 1) * DH] for h in range(i * STACK, (i + 1) * STACK)], axis=0
        )
        peaks = [None] * STACK
        for b in range(blocks):
            s = lax.dot_general(
                q, keys[b][...], (((1,), (1,)), ((), ())), preferred_element_type=jnp.float32
            )
            for g in range(STACK):
                part = s[g * rows : (g + 1) * rows] + bias_ref[:, b * rows : (b + 1) * rows]
                s_ref[i * STACK + g, :, b * rows : (b + 1) * rows] = part
                for c in range(0, rows, DH):
                    lanes = part[:, c : c + DH]
                    peaks[g] = lanes if peaks[g] is None else jnp.maximum(peaks[g], lanes)
        return [jnp.max(p, axis=1, keepdims=True) for p in peaks]

    def mix(i, peaks):
        total = None
        for b in range(blocks):
            p = jnp.concatenate(
                [
                    jnp.exp2(
                        (s_ref[i * STACK + g, :, b * rows : (b + 1) * rows] - peaks[g]) * factor
                    ).astype(jnp.bfloat16)
                    for g in range(STACK)
                ],
                axis=0,
            )
            v = jnp.concatenate([values[b][...], jnp.ones_like(values[b])], axis=1)
            o = jnp.dot(p, v, preferred_element_type=jnp.float32)
            total = o if total is None else total + o
        out = (total[:, :DH] / total[:, DH:]).astype(jnp.bfloat16)
        for g in range(STACK):
            h = i * STACK + g
            o_ref[:, h * DH : (h + 1) * DH] = out[g * rows : (g + 1) * rows]

    count = HEADS_PER_STEP // STACK
    peaks = scores(0)
    for i in range(count):
        later = scores(i + 1) if i + 1 < count else None
        mix(i, peaks)
        peaks = later


def attend(head, only, queries, bias, pieces, group_size, earlier):
    rows, width = queries.shape
    blocks = len(pieces)
    first = 0 if only is None else only
    count = pieces[0].shape[1] // DH if only is None else 1
    wide = HEADS_PER_STEP * DH
    per = group_size // HEADS_PER_STEP
    key_spec = pl.BlockSpec((rows, DH), lambda h, base: (0, first + h // per))
    value_spec = pl.BlockSpec((rows, DH), lambda h, base: (1, first + h // per))
    head_spec = pl.BlockSpec((rows, wide), lambda h, base: (0, base[0] * per + h))
    in_specs = [head_spec, pl.BlockSpec((rows, blocks * rows), lambda h, base: (0, 0))]
    in_specs += [key_spec] * blocks + [value_spec] * blocks
    operands = [queries, bias, *pieces, *pieces]
    aliases = {}
    if earlier is not None:
        in_specs.append(pl.BlockSpec(memory_space=pl.ANY))
        operands.append(earlier)
        aliases = {len(operands): 0}
    heads = count * group_size
    return pl.pallas_call(
        functools.partial(attend_kernel, math.log2(math.e) / math.sqrt(DH), blocks),
        grid_spec=pltpu.PrefetchScalarGridSpec(
            num_scalar_prefetch=1,
            grid=(count * per,),
            in_specs=in_specs,
            out_specs=head_spec,
            scratch_shapes=[pltpu.VMEM((HEADS_PER_STEP, rows, blocks * rows), jnp.float32)],
        ),
        out_shape=jax.ShapeDtypeStruct((rows, width), jnp.bfloat16),
        input_output_aliases=aliases,
        compiler_params=pltpu.CompilerParams(vmem_limit_bytes=60 * 2**20),
        cost_estimate=pl.CostEstimate(
            flops=4 * heads * rows * rows * blocks * DH,
            bytes_accessed=4 * rows * heads * DH + 4 * rows * rows * blocks,
            transcendentals=heads * rows * rows * blocks,
        ),
        name="attend",
    )(jnp.stack([head]), *operands)


def rotation(positions):
    half = DH // 2
    frequency = jnp.power(500000.0, -2.0 * jnp.arange(half, dtype=jnp.float32) / DH)
    angles = positions.astype(jnp.float32)[:, None] * frequency[None, :]
    cosine, sine = jnp.cos(angles), jnp.sin(angles)
    return (
        jnp.concatenate([cosine, cosine], axis=1),
        jnp.concatenate([-sine, sine], axis=1),
    )


def gather_line(side, piece, dy, dx, where):
    rows = piece.shape[0]
    before = torus_shift(piece, side, dy, dx)
    after = torus_shift(piece, side, -dy, -dx)
    three = jnp.concatenate([after, piece, before], axis=0)
    far_before = torus_shift(three, side, 3 * dy, 3 * dx)
    far_after = torus_shift(three[rows:], side, -3 * dy, -3 * dx)
    spans = ((0,), (1,), (-1,), (2, 3, 4), (-3, -2))
    return join(side, where, [piece, before, after, far_before, far_after], spans)


def next_stage(side, stage, dy, dx):
    half = side // 2
    if len(stage) == 1:
        forth = back = stage[0][1]
    else:
        (_, forth), (_, back) = stage
    k = abs(stage[0][0][0]) + 1
    if k < half:
        spans = ((k, 0, side), (-k, 0, side))
    else:
        rows = forth.shape[0] // 2
        forth, back = forth[:rows], back[rows:]
        spans = ((half, 0, half), (half, half, side))
    return [
        (spans[0], torus_shift(forth, side, dy, dx)),
        (spans[1], torus_shift(back, side, -dy, -dx)),
    ]


def hold(stage, *others):
    held = after([w for _, w in stage], *others)
    return [(span, w) for (span, _), w in zip(stage, held)]


def next_blocks(side, passed, other, first):
    if other is not None:
        other = start_backwards(other, side) if first else torus_shift(other, side, 0, -1)
    return next_on_dp(passed), other


def per_device(tokens, queries, w_key, w_value, lengths):
    tok_count = tokens.shape[0]
    side = ROW // tok_count
    assert side * side == lax.axis_size("dp") and lax.axis_size("groups") % 2 == 0
    assert lax.axis_size("mp") == 2 and ROW // 2 // tok_count == side // 2
    kv_local = w_key.shape[1] // DH
    group_size = queries.shape[1] // DH // kv_local
    half_width = w_key.shape[1] // 2
    place = lax.axis_index("dp")
    y, x, core = place // side, place % side, lax.axis_index("mp")
    part = lax.axis_index("groups") % 2

    tokens_z = group_swap(tokens)
    tokens_other = core_swap(tokens)

    key_piece = lax.dynamic_slice_in_dim(w_key, part * half_width, half_width, 1)
    value_piece = lax.dynamic_slice_in_dim(w_value, part * half_width, half_width, 1)
    key_chunk = gather_line(side, key_piece, 0, 1, jnp.stack([x]))
    value_chunk = gather_line(side, value_piece, 1, 0, jnp.stack([y]))
    all_tokens = tok_count * lax.axis_size("dp")
    first_token = (place * tok_count - ROW // 2 + all_tokens) % all_tokens
    row_index = first_token // ROW
    row_lengths = lax.dynamic_slice_in_dim(lengths, row_index, 1, 0)[0]
    finish = jnp.cumsum(row_lengths)
    own_offsets = first_token - row_index * ROW + jnp.arange(tok_count, dtype=jnp.int32)
    before = finish[None, :] <= own_offsets[:, None]
    started = jnp.sum(jnp.where(before, row_lengths[None, :], 0), axis=1)
    positions = own_offsets - started
    tables = rotation(positions)
    positions_z = group_swap(positions)
    window = jnp.arange(side * tok_count, dtype=jnp.int32)
    key_offsets = own_offsets[0] - window // tok_count * tok_count + window % tok_count
    allowed = (key_offsets[None, :] >= started[:, None]) & (
        key_offsets[None, :] <= own_offsets[:, None]
    )
    bias = jnp.where(allowed, 0.0, NEG).astype(jnp.float32)

    own_set = (tokens, tokens_other)
    where = jnp.stack([y, x, core])
    half = side // 2
    ask = lambda *ks: ([c for k in ks for c in key[k]], [c for k in ks for c in value[k]])
    chunks = lambda k: [w for _, w in key[k] + value[k]]

    def advance():
        key.append(next_stage(side, key[-1], 1, 0))
        value.append(next_stage(side, value[-1], 0, 1))

    key, value = [[((0, 0, side), key_chunk)]], [[((0, 0, side), value_chunk)]]
    advance()
    *tables, bias = after([*tables, bias], key_chunk, value_chunk)
    key[1], value[1] = hold(key[1], *tables, bias), hold(value[1], *tables, bias)
    advance()
    (own_sum,) = project(side, where, [ask(0, 1)], [own_set], [None])
    key[2], value[2] = hold(key[2], own_sum[0]), hold(value[2], own_sum[0])
    (tokens_z,) = after([tokens_z], *chunks(2))
    tokens_z_other = core_swap(tokens_z)
    z_set = (tokens_z, tokens_z_other)
    (positions_z,) = after([positions_z], tokens_z)
    tables_z = rotation(positions_z)
    advance()
    own_sum, z_sum = project(
        side, where, [ask(2), ask(0, 1, 2)], [own_set, z_set], [own_sum, None]
    )
    key[3], value[3] = hold(key[3], z_sum[0], *tables_z), hold(value[3], z_sum[0], *tables_z)
    advance()
    own_sum, z_sum = project(
        side, where, [ask(3), ask(3)], [own_set, z_set], [own_sum, z_sum]
    )
    kv_own, kv_z = project(
        side,
        where,
        [ask(half), ask(half)],
        [own_set, z_set],
        [own_sum, z_sum],
        [tables, tables_z],
    )
    kv_back = group_swap(kv_z)

    kept, back = [[kv_own], []], [[kv_back], []]
    passed, other = kv_own, kv_own
    passed_b, other_b = kv_back, kv_back
    own_step = part * (kv_local // 2)
    out = None
    for k in range(half):
        more = k < half - 1
        passed, other = next_blocks(side, passed, other if more else None, k == 0)
        kept[0].append(passed)
        if more:
            kept[1].insert(0, other)
        if k > 0:
            passed_b, other_b = next_blocks(side, passed_b, other_b, k == 1)
            back[0].append(passed_b)
            back[1].insert(0, other_b)
    pieces = kept[0] + kept[1]
    out = attend(own_step, 0, queries, bias, pieces, group_size, None)
    passed_b, held = after([passed_b, out])
    passed_b, _ = next_blocks(side, passed_b, None, False)
    out = attend(own_step + 1, 1, queries, bias, pieces, group_size, held)
    back[0].append(passed_b)
    pieces = back[0] + back[1]
    other_step = (1 - part) * (kv_local // 2)
    return attend(other_step, None, queries, bias, pieces, group_size, out)


def solution(mesh):
    return jax.shard_map(
        per_device,
        mesh=mesh,
        in_specs=(
            P(("groups", "dp"), "mp"),
            P(("groups", "dp"), "mp"),
            P("dp", "mp"),
            P("dp", "mp"),
            P("groups", None),
        ),
        out_specs=P(("groups", "dp"), "mp"),
        check_vma=False,
    )
```

```python
import functools
import math

import jax
import jax.numpy as jnp
from jax import lax
from jax.experimental import pallas as pl
from jax.experimental.pallas import tpu as pltpu
from jax.sharding import PartitionSpec as P

DH = 128
ROW = 2048
HEADS_PER_STEP = 4
STACK = 2
NEG = -1e30


def torus_shift(block, side, dy, dx):
    route = []
    for y in range(side):
        for x in range(side):
            route.append((y * side + x, (y + dy) % side * side + (x + dx) % side))
    return lax.ppermute(block, "dp", route)


def start_backwards(block, side):
    route = []
    for y in range(side):
        for x in range(side):
            down = 1 if x >= side // 2 else 0
            route.append((y * side + x, (y + down) % side * side + (x - 1) % side))
    return lax.ppermute(block, "dp", route)


def next_on_dp(block):
    count = lax.axis_size("dp")
    return lax.ppermute(block, "dp", [(i, (i + 1) % count) for i in range(count)])


def after(values, *others):
    held = lax.optimization_barrier((tuple(values), tuple(others)))
    return list(held[0])


def group_swap(block):
    count = lax.axis_size("groups")
    return lax.ppermute(block, "groups", [(i, i ^ 1) for i in range(count)])


def core_swap(block):
    return lax.ppermute(block, "mp", [(0, 1), (1, 0)])


def join_kernel(side, spans, where_ref, *refs):
    pieces, out, sems = refs[:-2], refs[-2], refs[-1]
    own = where_ref[0]
    rows = out.shape[0] // side
    copies = []
    for piece, shifts in zip(pieces, spans):
        for k, shift in enumerate(shifts):
            source = lax.rem(own - shift + 2 * side, side)
            target = out.at[pl.ds(pl.multiple_of(source * rows, rows), rows), :]
            copies.append(
                pltpu.make_async_copy(
                    piece.at[pl.ds(k * rows, rows), :], target, sems.at[len(copies)]
                )
            )
    for copy in copies:
        copy.start()
    for copy in copies:
        copy.wait()


def join(side, own, pieces, spans):
    columns = pieces[0].shape[1]
    rows = pieces[0].shape[0] // len(spans[0])
    return pl.pallas_call(
        functools.partial(join_kernel, side, spans),
        in_specs=[pl.BlockSpec(memory_space=pltpu.SMEM)]
        + [pl.BlockSpec(memory_space=pl.ANY)] * len(pieces),
        out_specs=pl.BlockSpec(memory_space=pltpu.VMEM),
        out_shape=jax.ShapeDtypeStruct((side * rows, columns), pieces[0].dtype),
        scratch_shapes=[pltpu.SemaphoreType.DMA((side,))],
        compiler_params=pltpu.CompilerParams(vmem_limit_bytes=60 * 2**20),
        cost_estimate=pl.CostEstimate(
            flops=10**6, bytes_accessed=4 * side * rows * columns, transcendentals=0
        ),
        name="join",
    )(own, *pieces)


def project_kernel(side, work, has_sums, final, where_ref, *refs):
    refs = list(refs)
    take = lambda n: [refs.pop(0) for _ in range(n)]
    count = 1 + max(item[0] for keys, values in work for item in keys + values)
    weights = take(count)
    tokens = [take(2) for _ in work]
    sums = [take(2) if has_sums[s] else None for s in range(len(work))]
    tables = [take(2) for _ in work] if final else None
    staged, sems = refs[-2], refs[-1]
    outs = refs[:-2]
    y, x, core = where_ref[0], where_ref[1], where_ref[2]
    half = side // 2
    unit = tokens[0][0].shape[1] // half
    piece = unit // side
    slot, sem = 0, 0
    plan = []
    for s, (keys, values) in enumerate(work):
        own, other = tokens[s]

        def bring(source_half, start, width, slot, lane, sem):
            target = staged.at[slot, :, pl.ds(lane, width)]
            window = pl.ds(pl.multiple_of(start, piece), width)
            for array, test in ((own, source_half == core), (other, source_half != core)):

                @pl.when(test)
                def _():
                    pltpu.make_async_copy(array.at[:, window], target, sems.at[sem]).start()

            return pltpu.make_async_copy(own.at[:, window], target, sems.at[sem])

        for which, items in enumerate((keys, values)):
            for operand, shift, lo, hi in items:
                waits = []
                if which == 0:
                    row = lax.rem(y - shift + 2 * side, side)
                    start = lax.rem(row, half) * unit + lo * piece
                    waits.append(
                        bring(lax.div(row, half), start, (hi - lo) * piece, slot, 0, sem)
                    )
                    sem += 1
                else:
                    column = lax.rem(x - shift + 2 * side, side)
                    for k, row in enumerate(range(lo, hi)):
                        start = (row % half) * unit + column * piece
                        waits.append(
                            bring(row // half, start, piece, slot, k * piece, sem)
                        )
                        sem += 1
                plan.append((s, which, operand, slot, (hi - lo) * piece, waits))
                slot += 1
    totals = [[r[...] for r in sums[s]] if sums[s] else [None, None] for s in range(len(work))]
    for s, which, operand, slot, depth, waits in plan:
        for wait in waits:
            wait.wait()
        product = jnp.dot(
            staged[slot, :, :depth], weights[operand][...], preferred_element_type=jnp.float32
        )
        old = totals[s][which]
        totals[s][which] = product if old is None else old + product
    rows = staged.shape[1]
    for s in range(len(work)):
        key_sum, value_sum = totals[s]
        if not final:
            outs[2 * s][...] = key_sum
            outs[2 * s + 1][...] = value_sum
            continue
        cosine, sine = tables[s][0][...], tables[s][1][...]
        for h in range(key_sum.shape[1] // DH):
            k = key_sum[:, h * DH : (h + 1) * DH]
            turned = jnp.concatenate([k[:, DH // 2 :], k[:, : DH // 2]], axis=1)
            outs[s][:rows, h * DH : (h + 1) * DH] = (k * cosine + turned * sine).astype(
                jnp.bfloat16
            )
        outs[s][rows:, :] = value_sum.astype(jnp.bfloat16)


def project(side, where, work, tokens, sums, tables=None):
    rows = tokens[0][0].shape[0]
    arrays, names = [], []
    for keys, values in work:
        plan = []
        for items in (keys, values):
            plan.append([])
            for (shift, lo, hi), w in items:
                at = next((k for k, a in enumerate(arrays) if a is w), None)
                if at is None:
                    at = len(arrays)
                    arrays.append(w)
                plan[-1].append((at, shift, lo, hi))
        names.append(tuple(plan))
    width = arrays[0].shape[1]
    operands = list(arrays)
    specs = [pl.BlockSpec(memory_space=pltpu.VMEM)] * len(arrays)
    for pair in tokens:
        operands += list(pair)
        specs += [pl.BlockSpec(memory_space=pl.ANY)] * 2
    for pair in list(sums) + list(tables or []):
        if pair is not None:
            operands += list(pair)
            specs += [pl.BlockSpec(memory_space=pltpu.VMEM)] * 2
    if tables is not None:
        shapes = [jax.ShapeDtypeStruct((2 * rows, width), jnp.bfloat16)] * len(work)
    else:
        shapes = [jax.ShapeDtypeStruct((rows, width), jnp.float32)] * (2 * len(work))
    items = [i for keys, values in names for i in keys + values]
    copies = sum(len(keys) + sum(i[3] - i[2] for i in values) for keys, values in names)
    depth = max(a.shape[0] for a in arrays)
    out = pl.pallas_call(
        functools.partial(
            project_kernel, side, names, [p is not None for p in sums], tables is not None
        ),
        in_specs=[pl.BlockSpec(memory_space=pltpu.SMEM)] + specs,
        out_specs=[pl.BlockSpec(memory_space=pltpu.VMEM)] * len(shapes),
        out_shape=shapes,
        scratch_shapes=[
            pltpu.VMEM((len(items), rows, depth), jnp.bfloat16),
            pltpu.SemaphoreType.DMA((copies,)),
        ],
        compiler_params=pltpu.CompilerParams(vmem_limit_bytes=16 * 2**20),
        cost_estimate=pl.CostEstimate(
            flops=2 * rows * depth * width * len(items),
            bytes_accessed=len(items) * depth * (rows + width) * 2,
            transcendentals=0,
        ),
        name="project",
    )(where, *operands)
    if tables is not None:
        return list(out)
    return [(out[2 * s], out[2 * s + 1]) for s in range(len(work))]


def attend_kernel(factor, blocks, base_ref, q_ref, sequence_ref, others_ref, causal_ref, *refs):
    keys, values = refs[:blocks], refs[blocks : 2 * blocks]
    o_ref, s_ref = refs[-2], refs[-1]
    rows = q_ref.shape[0]

    def scores(i):
        q = jnp.concatenate(
            [q_ref[:, h * DH : (h + 1) * DH] for h in range(i * STACK, (i + 1) * STACK)], axis=0
        )
        q = jnp.concatenate([q, jnp.concatenate([sequence_ref[...]] * STACK, axis=0)], axis=1)
        peaks = [None] * STACK
        for b in range(blocks):
            others = others_ref[b * rows : (b + 1) * rows, :]
            s = lax.dot_general(
                q,
                jnp.concatenate([keys[b][...], others], axis=1),
                (((1,), (1,)), ((), ())),
                preferred_element_type=jnp.float32,
            )
            for g in range(STACK):
                part = s[g * rows : (g + 1) * rows]
                if b == 0:
                    part = part + causal_ref[...]
                s_ref[i * STACK + g, :, b * rows : (b + 1) * rows] = part
                for c in range(0, rows, DH):
                    lanes = part[:, c : c + DH]
                    peaks[g] = lanes if peaks[g] is None else jnp.maximum(peaks[g], lanes)
        return [jnp.max(p, axis=1, keepdims=True) for p in peaks]

    def mix(i, peaks):
        total = None
        for b in range(blocks):
            p = jnp.concatenate(
                [
                    jnp.exp2(
                        (s_ref[i * STACK + g, :, b * rows : (b + 1) * rows] - peaks[g]) * factor
                    ).astype(jnp.bfloat16)
                    for g in range(STACK)
                ],
                axis=0,
            )
            v = jnp.concatenate([values[b][...], jnp.ones_like(values[b])], axis=1)
            o = jnp.dot(p, v, preferred_element_type=jnp.float32)
            total = o if total is None else total + o
        out = (total[:, :DH] / total[:, DH:]).astype(jnp.bfloat16)
        for g in range(STACK):
            h = i * STACK + g
            o_ref[:, h * DH : (h + 1) * DH] = out[g * rows : (g + 1) * rows]

    count = HEADS_PER_STEP // STACK
    peaks = scores(0)
    for i in range(count):
        later = scores(i + 1) if i + 1 < count else None
        mix(i, peaks)
        peaks = later


def attend(head, queries, masks, pieces, group_size, earlier=None):
    rows, width = queries.shape
    blocks = len(pieces)
    count = pieces[0].shape[1] // DH
    wide = HEADS_PER_STEP * DH
    per = group_size // HEADS_PER_STEP
    key_spec = pl.BlockSpec((rows, DH), lambda h, base: (0, h // per))
    value_spec = pl.BlockSpec((rows, DH), lambda h, base: (1, h // per))
    head_spec = pl.BlockSpec((rows, wide), lambda h, base: (0, base[0] * per + h))
    in_specs = [head_spec] + [pl.BlockSpec(m.shape, lambda h, base: (0, 0)) for m in masks]
    in_specs += [key_spec] * blocks + [value_spec] * blocks
    operands = [queries, *masks, *pieces, *pieces]
    aliases = {}
    if earlier is not None:
        in_specs.append(pl.BlockSpec(memory_space=pl.ANY))
        operands.append(earlier)
        aliases = {len(operands): 0}
    heads = count * group_size
    return pl.pallas_call(
        functools.partial(attend_kernel, math.log2(math.e) / math.sqrt(DH), blocks),
        grid_spec=pltpu.PrefetchScalarGridSpec(
            num_scalar_prefetch=1,
            grid=(count * per,),
            in_specs=in_specs,
            out_specs=head_spec,
            scratch_shapes=[pltpu.VMEM((HEADS_PER_STEP, rows, blocks * rows), jnp.float32)],
        ),
        out_shape=jax.ShapeDtypeStruct((rows, width), jnp.bfloat16),
        input_output_aliases=aliases,
        compiler_params=pltpu.CompilerParams(vmem_limit_bytes=60 * 2**20),
        cost_estimate=pl.CostEstimate(
            flops=4 * heads * rows * rows * blocks * DH,
            bytes_accessed=4 * rows * heads * DH + 4 * rows * rows * blocks,
            transcendentals=heads * rows * rows * blocks,
        ),
        name="attend",
    )(jnp.stack([head]), *operands)


def rotation(positions):
    half = DH // 2
    frequency = jnp.power(500000.0, -2.0 * jnp.arange(half, dtype=jnp.float32) / DH)
    angles = positions.astype(jnp.float32)[:, None] * frequency[None, :]
    cosine, sine = jnp.cos(angles), jnp.sin(angles)
    return (
        jnp.concatenate([cosine, cosine], axis=1),
        jnp.concatenate([-sine, sine], axis=1),
    )


def gather_line(side, piece, dy, dx, where):
    rows = piece.shape[0]
    before = torus_shift(piece, side, dy, dx)
    after = torus_shift(piece, side, -dy, -dx)
    three = jnp.concatenate([after, piece, before], axis=0)
    far_before = torus_shift(three, side, 3 * dy, 3 * dx)
    far_after = torus_shift(three[rows:], side, -3 * dy, -3 * dx)
    spans = ((0,), (1,), (-1,), (2, 3, 4), (-3, -2))
    return join(side, where, [piece, before, after, far_before, far_after], spans)


def next_stage(side, stage, dy, dx):
    half = side // 2
    if len(stage) == 1:
        forth = back = stage[0][1]
    else:
        (_, forth), (_, back) = stage
    k = abs(stage[0][0][0]) + 1
    if k < half:
        spans = ((k, 0, side), (-k, 0, side))
    else:
        rows = forth.shape[0] // 2
        forth, back = forth[:rows], back[rows:]
        spans = ((half, 0, half), (half, half, side))
    return [
        (spans[0], torus_shift(forth, side, dy, dx)),
        (spans[1], torus_shift(back, side, -dy, -dx)),
    ]


def hold(stage, *others):
    held = after([w for _, w in stage], *others)
    return [(span, w) for (span, _), w in zip(stage, held)]


def next_blocks(side, passed, other, first):
    if other is not None:
        other = start_backwards(other, side) if first else torus_shift(other, side, 0, -1)
    return next_on_dp(passed), other


def per_device(tokens, queries, w_key, w_value, lengths):
    tok_count = tokens.shape[0]
    side = ROW // tok_count
    assert side * side == lax.axis_size("dp") and lax.axis_size("groups") % 2 == 0
    assert lax.axis_size("mp") == 2 and ROW // 2 // tok_count == side // 2
    kv_local = w_key.shape[1] // DH
    group_size = queries.shape[1] // DH // kv_local
    half_width = w_key.shape[1] // 2
    place = lax.axis_index("dp")
    y, x, core = place // side, place % side, lax.axis_index("mp")
    part = lax.axis_index("groups") % 2

    tokens_z = group_swap(tokens)
    tokens_other = core_swap(tokens)

    key_piece = lax.dynamic_slice_in_dim(w_key, part * half_width, half_width, 1)
    value_piece = lax.dynamic_slice_in_dim(w_value, part * half_width, half_width, 1)
    key_chunk = gather_line(side, key_piece, 0, 1, jnp.stack([x]))
    value_chunk = gather_line(side, value_piece, 1, 0, jnp.stack([y]))
    all_tokens = tok_count * lax.axis_size("dp")
    first_token = (place * tok_count - ROW // 2 + all_tokens) % all_tokens
    row_index = first_token // ROW
    (lengths,) = after([lengths], key_chunk, value_chunk)
    row_lengths = lax.dynamic_slice_in_dim(lengths, row_index, 1, 0)[0]
    finish = jnp.cumsum(row_lengths)
    own_offsets = first_token - row_index * ROW + jnp.arange(tok_count, dtype=jnp.int32)
    before = finish[None, :] <= own_offsets[:, None]
    started = jnp.sum(jnp.where(before, row_lengths[None, :], 0), axis=1)
    positions = own_offsets - started
    tables = rotation(positions)
    positions_z = group_swap(positions)
    window = jnp.arange(side * tok_count, dtype=jnp.int32)
    key_offsets = own_offsets[0] - window // tok_count * tok_count + window % tok_count
    spare = DH - row_lengths.shape[0]
    ends = jnp.pad(finish, (0, spare), constant_values=-1)[None, :]
    begins = jnp.pad(finish - row_lengths, (0, spare))[None, :]
    belongs = lambda offsets: (offsets[:, None] >= begins) & (offsets[:, None] < ends)
    sequence = jnp.where(belongs(own_offsets), 1.0, 0.0).astype(jnp.bfloat16)
    others = jnp.where(belongs(key_offsets), 0.0, NEG).astype(jnp.bfloat16)
    within = jnp.arange(tok_count, dtype=jnp.int32)
    causal = jnp.where(within[None, :] <= within[:, None], 0.0, NEG).astype(jnp.float32)

    own_set = (tokens, tokens_other)
    where = jnp.stack([y, x, core])
    half = side // 2
    ask = lambda *ks: ([c for k in ks for c in key[k]], [c for k in ks for c in value[k]])
    chunks = lambda k: [w for _, w in key[k] + value[k]]

    def advance():
        key.append(next_stage(side, key[-1], 1, 0))
        value.append(next_stage(side, value[-1], 0, 1))

    key, value = [[((0, 0, side), key_chunk)]], [[((0, 0, side), value_chunk)]]
    advance()
    *tables, sequence, others, causal = after(
        [*tables, sequence, others, causal], key_chunk, value_chunk
    )
    masks = [sequence, others, causal]
    key[1], value[1] = hold(key[1], *tables, *masks), hold(value[1], *tables, *masks)
    advance()
    (own_sum,) = project(side, where, [ask(0, 1)], [own_set], [None])
    key[2], value[2] = hold(key[2], own_sum[0]), hold(value[2], own_sum[0])
    (tokens_z,) = after([tokens_z], *chunks(2))
    tokens_z_other = core_swap(tokens_z)
    z_set = (tokens_z, tokens_z_other)
    (positions_z,) = after([positions_z], tokens_z)
    tables_z = rotation(positions_z)
    advance()
    own_sum, z_sum = project(
        side, where, [ask(2), ask(0, 1, 2)], [own_set, z_set], [own_sum, None]
    )
    key[3], value[3] = hold(key[3], z_sum[0], *tables_z), hold(value[3], z_sum[0], *tables_z)
    advance()
    own_sum, z_sum = project(
        side, where, [ask(3), ask(3)], [own_set, z_set], [own_sum, z_sum]
    )
    kv_own, kv_z = project(
        side,
        where,
        [ask(half), ask(half)],
        [own_set, z_set],
        [own_sum, z_sum],
        [tables, tables_z],
    )
    kv_back = group_swap(kv_z)

    kept, back = [[kv_own], []], [[kv_back], []]
    passed, other = kv_own, kv_own
    passed_b, other_b = kv_back, kv_back
    for k in range(half):
        more = k < half - 1
        passed, other = next_blocks(side, passed, other if more else None, k == 0)
        if not more:
            (passed_b,) = after([passed_b], passed)
        passed_b, other_b = next_blocks(side, passed_b, other_b if more else None, k == 0)
        kept[0].append(passed)
        back[0].append(passed_b)
        if more:
            kept[1].insert(0, other)
            back[1].insert(0, other_b)
    own_head, other_head = part * (kv_local // 2), (1 - part) * (kv_local // 2)
    out = attend(own_head, queries, masks, kept[0] + kept[1], group_size)
    return attend(other_head, queries, masks, back[0] + back[1], group_size, out)


def solution(mesh):
    return jax.shard_map(
        per_device,
        mesh=mesh,
        in_specs=(
            P(("groups", "dp"), "mp"),
            P(("groups", "dp"), "mp"),
            P("dp", "mp"),
            P("dp", "mp"),
            P("groups", None),
        ),
        out_specs=P(("groups", "dp"), "mp"),
        check_vma=False,
    )
```

```python
import functools
import math

import jax
import jax.numpy as jnp
from jax import lax
from jax.experimental import pallas as pl
from jax.experimental.pallas import tpu as pltpu
from jax.sharding import PartitionSpec as P

DH = 128
ROW = 2048
HEADS_PER_STEP = 4
STACK = 2
NEG = -1e30


def torus_shift(block, side, dy, dx):
    route = []
    for y in range(side):
        for x in range(side):
            route.append((y * side + x, (y + dy) % side * side + (x + dx) % side))
    return lax.ppermute(block, "dp", route)


def start_backwards(block, side):
    route = []
    for y in range(side):
        for x in range(side):
            down = 1 if x >= side // 2 else 0
            route.append((y * side + x, (y + down) % side * side + (x - 1) % side))
    return lax.ppermute(block, "dp", route)


def next_on_dp(block):
    count = lax.axis_size("dp")
    return lax.ppermute(block, "dp", [(i, (i + 1) % count) for i in range(count)])


def after(values, *others):
    held = lax.optimization_barrier((tuple(values), tuple(others)))
    return list(held[0])


def group_swap(block):
    count = lax.axis_size("groups")
    return lax.ppermute(block, "groups", [(i, i ^ 1) for i in range(count)])


def core_swap(block):
    return lax.ppermute(block, "mp", [(0, 1), (1, 0)])


def join_kernel(side, spans, where_ref, *refs):
    pieces, out, sems = refs[:-2], refs[-2], refs[-1]
    own = where_ref[0]
    rows = out.shape[0] // side
    copies = []
    for piece, shifts in zip(pieces, spans):
        for k, shift in enumerate(shifts):
            source = lax.rem(own - shift + 2 * side, side)
            target = out.at[pl.ds(pl.multiple_of(source * rows, rows), rows), :]
            copies.append(
                pltpu.make_async_copy(
                    piece.at[pl.ds(k * rows, rows), :], target, sems.at[len(copies)]
                )
            )
    for copy in copies:
        copy.start()
    for copy in copies:
        copy.wait()


def join(side, own, pieces, spans):
    columns = pieces[0].shape[1]
    rows = pieces[0].shape[0] // len(spans[0])
    return pl.pallas_call(
        functools.partial(join_kernel, side, spans),
        in_specs=[pl.BlockSpec(memory_space=pltpu.SMEM)]
        + [pl.BlockSpec(memory_space=pl.ANY)] * len(pieces),
        out_specs=pl.BlockSpec(memory_space=pltpu.VMEM),
        out_shape=jax.ShapeDtypeStruct((side * rows, columns), pieces[0].dtype),
        scratch_shapes=[pltpu.SemaphoreType.DMA((side,))],
        compiler_params=pltpu.CompilerParams(vmem_limit_bytes=60 * 2**20),
        cost_estimate=pl.CostEstimate(
            flops=10**6, bytes_accessed=4 * side * rows * columns, transcendentals=0
        ),
        name="join",
    )(own, *pieces)


def project_kernel(side, work, has_sums, final, where_ref, *refs):
    refs = list(refs)
    take = lambda n: [refs.pop(0) for _ in range(n)]
    count = 1 + max(item[0] for keys, values in work for item in keys + values)
    weights = take(count)
    tokens = [take(2) for _ in work]
    sums = [take(2) if has_sums[s] else None for s in range(len(work))]
    tables = [take(2) for _ in work] if final else None
    staged, sems = refs[-2], refs[-1]
    outs = refs[:-2]
    y, x, core = where_ref[0], where_ref[1], where_ref[2]
    half = side // 2
    rows = tokens[0][0].shape[0]
    unit = tokens[0][0].shape[1] // half
    piece = unit // side
    joint = len(work) > 1 and all(part == work[0] for part in work)
    slot, sem = 0, 0
    plan = []
    for s, (keys, values) in enumerate(work):
        own, other = tokens[s]
        slot = 0 if joint else slot
        base = s * rows if joint else 0

        def bring(source_half, start, width, slot, lane, sem):
            target = staged.at[slot, pl.ds(base, rows), pl.ds(lane, width)]
            window = pl.ds(pl.multiple_of(start, piece), width)
            for array, test in ((own, source_half == core), (other, source_half != core)):

                @pl.when(test)
                def _():
                    pltpu.make_async_copy(array.at[:, window], target, sems.at[sem]).start()

            return pltpu.make_async_copy(own.at[:, window], target, sems.at[sem])

        for which, items in enumerate((keys, values)):
            for operand, shift, lo, hi in items:
                waits = []
                if which == 0:
                    row = lax.rem(y - shift + 2 * side, side)
                    start = lax.rem(row, half) * unit + lo * piece
                    waits.append(
                        bring(lax.div(row, half), start, (hi - lo) * piece, slot, 0, sem)
                    )
                    sem += 1
                else:
                    column = lax.rem(x - shift + 2 * side, side)
                    for k, row in enumerate(range(lo, hi)):
                        start = (row % half) * unit + column * piece
                        waits.append(
                            bring(row // half, start, piece, slot, k * piece, sem)
                        )
                        sem += 1
                plan.append((s, which, operand, slot, (hi - lo) * piece, waits))
                slot += 1
    totals = [[r[...] for r in sums[s]] if sums[s] else [None, None] for s in range(len(work))]
    if joint:
        count = len(plan) // len(work)
        for i, (s, which, operand, slot, depth, _) in enumerate(plan[:count]):
            for step in plan[i::count]:
                for wait in step[-1]:
                    wait.wait()
            product = jnp.dot(
                staged[slot, :, :depth], weights[operand][...], preferred_element_type=jnp.float32
            )
            for k in range(len(work)):
                part = product[k * rows : (k + 1) * rows]
                old = totals[k][which]
                totals[k][which] = part if old is None else old + part
        plan = []
    for s, which, operand, slot, depth, waits in plan:
        for wait in waits:
            wait.wait()
        product = jnp.dot(
            staged[slot, :, :depth], weights[operand][...], preferred_element_type=jnp.float32
        )
        old = totals[s][which]
        totals[s][which] = product if old is None else old + product
    for s in range(len(work)):
        key_sum, value_sum = totals[s]
        if not final:
            outs[2 * s][...] = key_sum
            outs[2 * s + 1][...] = value_sum
            continue
        cosine, sine = tables[s][0][...], tables[s][1][...]
        for h in range(key_sum.shape[1] // DH):
            k = key_sum[:, h * DH : (h + 1) * DH]
            turned = jnp.concatenate([k[:, DH // 2 :], k[:, : DH // 2]], axis=1)
            outs[s][:rows, h * DH : (h + 1) * DH] = (k * cosine + turned * sine).astype(
                jnp.bfloat16
            )
        outs[s][rows:, :] = value_sum.astype(jnp.bfloat16)


def project(side, where, work, tokens, sums, tables=None):
    rows = tokens[0][0].shape[0]
    arrays, names = [], []
    for keys, values in work:
        plan = []
        for items in (keys, values):
            plan.append([])
            for (shift, lo, hi), w in items:
                at = next((k for k, a in enumerate(arrays) if a is w), None)
                if at is None:
                    at = len(arrays)
                    arrays.append(w)
                plan[-1].append((at, shift, lo, hi))
        names.append(tuple(plan))
    width = arrays[0].shape[1]
    operands = list(arrays)
    specs = [pl.BlockSpec(memory_space=pltpu.VMEM)] * len(arrays)
    for pair in tokens:
        operands += list(pair)
        specs += [pl.BlockSpec(memory_space=pl.ANY)] * 2
    for pair in list(sums) + list(tables or []):
        if pair is not None:
            operands += list(pair)
            specs += [pl.BlockSpec(memory_space=pltpu.VMEM)] * 2
    if tables is not None:
        shapes = [jax.ShapeDtypeStruct((2 * rows, width), jnp.bfloat16)] * len(work)
    else:
        shapes = [jax.ShapeDtypeStruct((rows, width), jnp.float32)] * (2 * len(work))
    items = [i for keys, values in names for i in keys + values]
    copies = sum(len(keys) + sum(i[3] - i[2] for i in values) for keys, values in names)
    depth = max(a.shape[0] for a in arrays)
    joint = len(work) > 1 and all(part == names[0] for part in names)
    staged = (len(items) // len(work), len(work) * rows) if joint else (len(items), rows)
    out = pl.pallas_call(
        functools.partial(
            project_kernel, side, names, [p is not None for p in sums], tables is not None
        ),
        in_specs=[pl.BlockSpec(memory_space=pltpu.SMEM)] + specs,
        out_specs=[pl.BlockSpec(memory_space=pltpu.VMEM)] * len(shapes),
        out_shape=shapes,
        scratch_shapes=[
            pltpu.VMEM((*staged, depth), jnp.bfloat16),
            pltpu.SemaphoreType.DMA((copies,)),
        ],
        compiler_params=pltpu.CompilerParams(vmem_limit_bytes=16 * 2**20),
        cost_estimate=pl.CostEstimate(
            flops=2 * rows * depth * width * len(items),
            bytes_accessed=len(items) * depth * (rows + width) * 2,
            transcendentals=0,
        ),
        name="project",
    )(where, *operands)
    if tables is not None:
        return list(out)
    return [(out[2 * s], out[2 * s + 1]) for s in range(len(work))]


def attend_kernel(factor, blocks, base_ref, q_ref, sequence_ref, others_ref, causal_ref, *refs):
    keys, values = refs[:blocks], refs[blocks : 2 * blocks]
    o_ref, s_ref = refs[-2], refs[-1]
    rows = q_ref.shape[0]

    def scores(i):
        q = jnp.concatenate(
            [q_ref[:, h * DH : (h + 1) * DH] for h in range(i * STACK, (i + 1) * STACK)], axis=0
        )
        q = jnp.concatenate([q, jnp.concatenate([sequence_ref[...]] * STACK, axis=0)], axis=1)
        peaks = [None] * STACK
        for b in range(blocks):
            others = others_ref[b * rows : (b + 1) * rows, :]
            s = lax.dot_general(
                q,
                jnp.concatenate([keys[b][...], others], axis=1),
                (((1,), (1,)), ((), ())),
                preferred_element_type=jnp.float32,
            )
            for g in range(STACK):
                part = s[g * rows : (g + 1) * rows]
                if b == 0:
                    part = part + causal_ref[...]
                s_ref[i * STACK + g, :, b * rows : (b + 1) * rows] = part
                for c in range(0, rows, DH):
                    lanes = part[:, c : c + DH]
                    peaks[g] = lanes if peaks[g] is None else jnp.maximum(peaks[g], lanes)
        return [jnp.max(p, axis=1, keepdims=True) for p in peaks]

    def mix(i, peaks):
        total = None
        for b in range(blocks):
            p = jnp.concatenate(
                [
                    jnp.exp2(
                        (s_ref[i * STACK + g, :, b * rows : (b + 1) * rows] - peaks[g]) * factor
                    ).astype(jnp.bfloat16)
                    for g in range(STACK)
                ],
                axis=0,
            )
            v = jnp.concatenate([values[b][...], jnp.ones_like(values[b])], axis=1)
            o = jnp.dot(p, v, preferred_element_type=jnp.float32)
            total = o if total is None else total + o
        out = (total[:, :DH] / total[:, DH:]).astype(jnp.bfloat16)
        for g in range(STACK):
            h = i * STACK + g
            o_ref[:, h * DH : (h + 1) * DH] = out[g * rows : (g + 1) * rows]

    count = HEADS_PER_STEP // STACK
    peaks = scores(0)
    for i in range(count):
        later = scores(i + 1) if i + 1 < count else None
        mix(i, peaks)
        peaks = later


def attend(head, queries, masks, pieces, group_size, earlier=None):
    rows, width = queries.shape
    blocks = len(pieces)
    count = pieces[0].shape[1] // DH
    wide = HEADS_PER_STEP * DH
    per = group_size // HEADS_PER_STEP
    key_spec = pl.BlockSpec((rows, DH), lambda h, base: (0, h // per))
    value_spec = pl.BlockSpec((rows, DH), lambda h, base: (1, h // per))
    head_spec = pl.BlockSpec((rows, wide), lambda h, base: (0, base[0] * per + h))
    in_specs = [head_spec] + [pl.BlockSpec(m.shape, lambda h, base: (0, 0)) for m in masks]
    in_specs += [key_spec] * blocks + [value_spec] * blocks
    operands = [queries, *masks, *pieces, *pieces]
    aliases = {}
    if earlier is not None:
        in_specs.append(pl.BlockSpec(memory_space=pl.ANY))
        operands.append(earlier)
        aliases = {len(operands): 0}
    heads = count * group_size
    return pl.pallas_call(
        functools.partial(attend_kernel, math.log2(math.e) / math.sqrt(DH), blocks),
        grid_spec=pltpu.PrefetchScalarGridSpec(
            num_scalar_prefetch=1,
            grid=(count * per,),
            in_specs=in_specs,
            out_specs=head_spec,
            scratch_shapes=[pltpu.VMEM((HEADS_PER_STEP, rows, blocks * rows), jnp.float32)],
        ),
        out_shape=jax.ShapeDtypeStruct((rows, width), jnp.bfloat16),
        input_output_aliases=aliases,
        compiler_params=pltpu.CompilerParams(vmem_limit_bytes=60 * 2**20),
        cost_estimate=pl.CostEstimate(
            flops=4 * heads * rows * rows * blocks * DH,
            bytes_accessed=4 * rows * heads * DH + 4 * rows * rows * blocks,
            transcendentals=heads * rows * rows * blocks,
        ),
        name="attend",
    )(jnp.stack([head]), *operands)


def rotation(positions):
    half = DH // 2
    frequency = jnp.power(500000.0, -2.0 * jnp.arange(half, dtype=jnp.float32) / DH)
    angles = positions.astype(jnp.float32)[:, None] * frequency[None, :]
    cosine, sine = jnp.cos(angles), jnp.sin(angles)
    return (
        jnp.concatenate([cosine, cosine], axis=1),
        jnp.concatenate([-sine, sine], axis=1),
    )


def gather_line(side, piece, dy, dx, where):
    rows = piece.shape[0]
    before = torus_shift(piece, side, dy, dx)
    after = torus_shift(piece, side, -dy, -dx)
    three = jnp.concatenate([after, piece, before], axis=0)
    far_before = torus_shift(three, side, 3 * dy, 3 * dx)
    far_after = torus_shift(three[rows:], side, -3 * dy, -3 * dx)
    spans = ((0,), (1,), (-1,), (2, 3, 4), (-3, -2))
    return join(side, where, [piece, before, after, far_before, far_after], spans)


def next_stage(side, stage, dy, dx):
    half = side // 2
    if len(stage) == 1:
        forth = back = stage[0][1]
    else:
        (_, forth), (_, back) = stage
    k = abs(stage[0][0][0]) + 1
    if k < half:
        spans = ((k, 0, side), (-k, 0, side))
    else:
        rows = forth.shape[0] // 2
        forth, back = forth[:rows], back[rows:]
        spans = ((half, 0, half), (half, half, side))
    return [
        (spans[0], torus_shift(forth, side, dy, dx)),
        (spans[1], torus_shift(back, side, -dy, -dx)),
    ]


def hold(stage, *others):
    held = after([w for _, w in stage], *others)
    return [(span, w) for (span, _), w in zip(stage, held)]


def next_blocks(side, passed, other, first):
    if other is not None:
        other = start_backwards(other, side) if first else torus_shift(other, side, 0, -1)
    return next_on_dp(passed), other


def per_device(tokens, queries, w_key, w_value, lengths):
    tok_count = tokens.shape[0]
    side = ROW // tok_count
    assert side * side == lax.axis_size("dp") and lax.axis_size("groups") % 2 == 0
    assert lax.axis_size("mp") == 2 and ROW // 2 // tok_count == side // 2
    kv_local = w_key.shape[1] // DH
    group_size = queries.shape[1] // DH // kv_local
    half_width = w_key.shape[1] // 2
    place = lax.axis_index("dp")
    y, x, core = place // side, place % side, lax.axis_index("mp")
    part = lax.axis_index("groups") % 2

    tokens_z = group_swap(tokens)
    tokens_other = core_swap(tokens)

    key_piece = lax.dynamic_slice_in_dim(w_key, part * half_width, half_width, 1)
    value_piece = lax.dynamic_slice_in_dim(w_value, part * half_width, half_width, 1)
    key_chunk = gather_line(side, key_piece, 0, 1, jnp.stack([x]))
    value_chunk = gather_line(side, value_piece, 1, 0, jnp.stack([y]))
    all_tokens = tok_count * lax.axis_size("dp")
    first_token = (place * tok_count - ROW // 2 + all_tokens) % all_tokens
    row_index = first_token // ROW
    (lengths,) = after([lengths], key_chunk, value_chunk)
    row_lengths = lax.dynamic_slice_in_dim(lengths, row_index, 1, 0)[0]
    finish = jnp.cumsum(row_lengths)
    own_offsets = first_token - row_index * ROW + jnp.arange(tok_count, dtype=jnp.int32)
    before = finish[None, :] <= own_offsets[:, None]
    started = jnp.sum(jnp.where(before, row_lengths[None, :], 0), axis=1)
    positions = own_offsets - started
    tables = rotation(positions)
    positions_z = group_swap(positions)
    window = jnp.arange(side * tok_count, dtype=jnp.int32)
    key_offsets = own_offsets[0] - window // tok_count * tok_count + window % tok_count
    spare = DH - row_lengths.shape[0]
    ends = jnp.pad(finish, (0, spare), constant_values=-1)[None, :]
    begins = jnp.pad(finish - row_lengths, (0, spare))[None, :]
    belongs = lambda offsets: (offsets[:, None] >= begins) & (offsets[:, None] < ends)
    sequence = jnp.where(belongs(own_offsets), 1.0, 0.0).astype(jnp.bfloat16)
    others = jnp.where(belongs(key_offsets), 0.0, NEG).astype(jnp.bfloat16)
    within = jnp.arange(tok_count, dtype=jnp.int32)
    causal = jnp.where(within[None, :] <= within[:, None], 0.0, NEG).astype(jnp.float32)

    own_set = (tokens, tokens_other)
    where = jnp.stack([y, x, core])
    half = side // 2
    ask = lambda *ks: ([c for k in ks for c in key[k]], [c for k in ks for c in value[k]])
    chunks = lambda k: [w for _, w in key[k] + value[k]]

    def advance():
        key.append(next_stage(side, key[-1], 1, 0))
        value.append(next_stage(side, value[-1], 0, 1))

    key, value = [[((0, 0, side), key_chunk)]], [[((0, 0, side), value_chunk)]]
    advance()
    *tables, sequence, others, causal = after(
        [*tables, sequence, others, causal], key_chunk, value_chunk
    )
    masks = [sequence, others, causal]
    key[1], value[1] = hold(key[1], *tables, *masks), hold(value[1], *tables, *masks)
    advance()
    (own_sum,) = project(side, where, [ask(0, 1)], [own_set], [None])
    key[2], value[2] = hold(key[2], own_sum[0]), hold(value[2], own_sum[0])
    (tokens_z,) = after([tokens_z], *chunks(2))
    tokens_z_other = core_swap(tokens_z)
    z_set = (tokens_z, tokens_z_other)
    (positions_z,) = after([positions_z], tokens_z)
    tables_z = rotation(positions_z)
    advance()
    own_sum, z_sum = project(
        side, where, [ask(2), ask(0, 1, 2)], [own_set, z_set], [own_sum, None]
    )
    key[3], value[3] = hold(key[3], z_sum[0], *tables_z), hold(value[3], z_sum[0], *tables_z)
    advance()
    own_sum, z_sum = project(
        side, where, [ask(3), ask(3)], [own_set, z_set], [own_sum, z_sum]
    )
    kv_own, kv_z = project(
        side,
        where,
        [ask(half), ask(half)],
        [own_set, z_set],
        [own_sum, z_sum],
        [tables, tables_z],
    )
    kv_back = group_swap(kv_z)

    kept, back = [[kv_own], []], [[kv_back], []]
    passed, other = kv_own, kv_own
    passed_b, other_b = kv_back, kv_back
    for k in range(half):
        more = k < half - 1
        passed, other = next_blocks(side, passed, other if more else None, k == 0)
        if not more:
            (passed_b,) = after([passed_b], passed)
        passed_b, other_b = next_blocks(side, passed_b, other_b if more else None, k == 0)
        kept[0].append(passed)
        back[0].append(passed_b)
        if more:
            kept[1].insert(0, other)
            back[1].insert(0, other_b)
    own_head, other_head = part * (kv_local // 2), (1 - part) * (kv_local // 2)
    out = attend(own_head, queries, masks, kept[0] + kept[1], group_size)
    return attend(other_head, queries, masks, back[0] + back[1], group_size, out)


def solution(mesh):
    return jax.shard_map(
        per_device,
        mesh=mesh,
        in_specs=(
            P(("groups", "dp"), "mp"),
            P(("groups", "dp"), "mp"),
            P("dp", "mp"),
            P("dp", "mp"),
            P("groups", None),
        ),
        out_specs=P(("groups", "dp"), "mp"),
        check_vma=False,
    )
```
